32 devices in a mesh: gx: 4 (over x, core), gy: 8 (over z, y).
Axes of the slice: x: 2, y: 2, z: 4, core: 2. Of those that a mesh axis runs over, the one named last changes fastest.
Arguments:
- feats: bfloat16 [1024, 128, 128], P(('gx', 'gy')), may hold values from -24 to 24
- z_count: int32 [32], P(('gx', 'gy')), may hold values from 8 to 32
- hil_dest: int32 [1024], P(('gx', 'gy')), may hold values from 0 to 1023, as said below
- pool_group: int32 [1024, 128], P(('gx', 'gy')), may hold values from 0 to 31, never falling along the last dimension, each value on 1 to 8 neighbouring positions
- z_qkv: bfloat16 [128, 384], replicated, may hold values from -9.0156115 to 9.0156115
- z_proj: bfloat16 [128, 128], replicated, may hold values from -0.5 to 0.5
- z_up: bfloat16 [128, 512], replicated, may hold values from -0.5 to 0.5
- z_down: bfloat16 [512, 128], replicated, may hold values from -0.25 to 0.25
- z_gain: float32 [2, 128], replicated, may hold values from 0.1 to 1.9
- pool_w: bfloat16 [128, 256], replicated, may hold values from -0.5 to 0.5
- bn_gain: float32 [256], replicated, may hold values from 0.1 to 1.9
- p_qkv: bfloat16 [256, 768], replicated, may hold values from -6.375 to 6.375
- p_proj: bfloat16 [256, 256], replicated, may hold values from -0.375 to 0.375
- p_up: bfloat16 [256, 1024], replicated, may hold values from -0.375 to 0.375
- p_down: bfloat16 [1024, 256], replicated, may hold values from -0.1875 to 0.1875
- p_gain: float32 [2, 256], replicated, may hold values from 0.1 to 1.9
- unpool_w: bfloat16 [256, 128], replicated, may hold values from -0.375 to 0.375
Outputs:
- out: bfloat16 [1024, 128, 128], P(('gx', 'gy'))
The draws below stay inside these ranges and needn't reach their ends.
Inputs may be any that keep to these rules, and one draw needn't show every extreme that they name: `hil_dest`: A permutation of 0 to 1023; value v stands for slot v % 32 of device v // 32, devices numbered gx index times the size of gy plus gy index. A cell stays on devices of its own gx index; of one device's 32 cells, each device of its gx index receives either none or exactly 8. `pool_group`: within each cell the numbers never fall, and each of 0 to 31 names 1 to 8 points.
All inputs are finite; a program needn't handle non-finite values.
Results may differ from the reference program's by a relative error of at most 0.018.
The reference program's roundings to bfloat16 on the way count: a program that leaves them out, or rounds other values in their place, can miss the bound.
Values may be sent and summed in bfloat16 or wider, within the bound.
A program may use at most 192 MiB of HBM per device.

```python
import math
import jax
import jax.numpy as jnp
import numpy as np
from jax import lax

C = 128
C2 = 256
HEAD = 16
CELL = 128
PGROUP = 32
CELL_DEV = 32
PATCH = 1024
NCELLS = 1024
CAP = 8
MOSTG = 8
N_GX = 4
N_GY = 8
DEVICES = 32


def draw_feats(key, part):
    device_count = N_GX * N_GY
    key_cells, key_values = jax.random.split(key, 2)
    owner = (jnp.arange(NCELLS) // CELL_DEV).astype(jnp.float32)
    fraction = owner / (device_count - 1)
    cell_scale = jnp.exp(jax.random.uniform(key_cells, (NCELLS,), minval=math.log(0.3), maxval=math.log(3.0)))
    ramp = jnp.exp(fraction * math.log(3.0)) / 1.7
    base = jnp.clip(jax.random.normal(key_values, (NCELLS, CELL, C)), -4.0, 4.0)
    return (base * (ramp * cell_scale)[:, None, None]).astype(jnp.bfloat16)


def one_permutation(single_key):
    return jax.random.permutation(single_key, CELL_DEV)


def one_row_routes(row_key):
    key_list = jax.random.split(row_key, 5)
    source_rank = jax.random.permutation(key_list[0], N_GY)
    target_order = jax.random.permutation(key_list[1], N_GY)
    offsets = jax.random.permutation(key_list[2], N_GY)[:N_GY // 2]
    cell_order = jax.vmap(one_permutation)(jax.random.split(key_list[3], N_GY))
    slot_order = jax.vmap(one_permutation)(jax.random.split(key_list[4], N_GY))
    target = target_order[(source_rank[:, None] + offsets[cell_order // CAP]) % N_GY]
    slot = slot_order[target, cell_order]
    return (target, slot)


def draw_hil_dest(key, part):
    targets, slots = jax.vmap(one_row_routes)(jax.random.split(key, N_GX))
    row_base = jnp.arange(N_GX, dtype=jnp.int32)[:, None, None] * N_GY
    return ((row_base + targets) * CELL_DEV + slots).reshape(-1).astype(jnp.int32)


def draw_z_qkv(key, part):
    drawn = jnp.clip(jax.random.normal(key, (C, 3 * C)), -4.0, 4.0) / math.sqrt(C)
    return drawn.astype(jnp.bfloat16)


def draw_p_qkv(key, part):
    drawn = jnp.clip(jax.random.normal(key, (C2, 3 * C2)), -4.0, 4.0) / math.sqrt(C2)
    return drawn.astype(jnp.bfloat16)


def set_ends(drawn, rng, least, top_value):
    index_at = [jax.random.randint(jax.random.fold_in(rng, axis), (), 0, length) for axis, length in enumerate(drawn.shape)]
    widest = drawn.shape.index(max(drawn.shape))
    neighbour = index_at[:widest] + [(index_at[widest] + 1) % drawn.shape[widest]] + index_at[widest + 1:]
    return drawn.at[tuple(index_at)].set(least).at[tuple(neighbour)].set(top_value)


def split_up(number_of, total, limit, slope):
    portions = [(1 << 20) // math.isqrt(grade ** slope) + 1 for grade in range(2, number_of + 1)]
    surplus, counts = total - limit - (number_of - 1), [1] * (number_of - 1)
    while surplus > 0:
        free = [i for i in range(number_of - 1) if counts[i] < limit]
        pool, budget = sum([portions[i] for i in free]), surplus
        for i in free:
            more = min(limit - counts[i], max(1, budget * portions[i] // pool), surplus)
            counts[i] = counts[i] + more
            surplus = surplus - more
    return np.array([limit] + counts)


def ragged_sizes(key, amount, total, reach, skew):
    if amount == 2:
        one = jax.random.randint(key, (), max(1, total - reach), min(reach, total - 1) + 1)
        return jnp.stack([one, total - one])
    lengths = jnp.asarray(split_up(amount, total, reach, skew), jnp.int32)
    twos = (amount - 1) // 2
    giver, sink = lengths[1:1 + 2 * twos:2], lengths[2:2 + 2 * twos:2]
    slack = jnp.minimum(giver - 1, reach - sink)
    shifted = jax.random.randint(jax.random.fold_in(key, 1), (twos,), 0, 1 << 20) % (slack + 1)
    lengths = lengths.at[1:1 + 2 * twos:2].set(giver - shifted).at[2:2 + 2 * twos:2].set(sink + shifted)
    return lengths[jax.random.permutation(jax.random.fold_in(key, 2), amount)]


def normal_values(rng, extent, scale, reach, kind=jnp.bfloat16):
    array = scale * jax.random.normal(rng, extent, jnp.float32)
    return jnp.clip(array, min=-reach, max=reach).astype(kind)


def setup_inputs(seed: int = 0) -> dict:
    splits = jax.random.split(jax.random.key(seed), 18)
    return {
        "feats": draw_feats(jax.random.fold_in(splits[17], 71), 0),
        "z_count": set_ends(jax.random.randint(splits[1], (DEVICES,), CELL_DEV // 4, CELL_DEV + 1), jax.random.fold_in(splits[1], 1), CELL_DEV // 4, CELL_DEV).astype(jnp.int32),
        "hil_dest": draw_hil_dest(jax.random.fold_in(splits[17], 71), 0),
        "pool_group": jax.vmap(lambda own: jnp.searchsorted(jnp.cumsum(ragged_sizes(own, PGROUP, CELL, MOSTG, 1)), jnp.arange(CELL), side="right"))(jax.random.split(splits[3], NCELLS)).reshape((NCELLS, CELL)).astype(jnp.int32),
        "z_qkv": draw_z_qkv(jax.random.fold_in(splits[17], 71), 0),
        "z_proj": normal_values(splits[5], (C, C), C ** -0.5, 0.5),
        "z_up": normal_values(splits[6], (C, 4 * C), C ** -0.5, 0.5),
        "z_down": normal_values(splits[7], (4 * C, C), (4 * C) ** -0.5, 0.25),
        "z_gain": jnp.clip(1.0 + 0.18 * jax.random.normal(splits[8], (2, C), jnp.float32), 0.1, 1.9),
        "pool_w": normal_values(splits[9], (C, C2), C ** -0.5, 0.5),
        "bn_gain": jnp.clip(1.0 + 0.18 * jax.random.normal(splits[10], (C2,), jnp.float32), 0.1, 1.9),
        "p_qkv": draw_p_qkv(jax.random.fold_in(splits[17], 71), 0),
        "p_proj": normal_values(splits[12], (C2, C2), C2 ** -0.5, 0.375),
        "p_up": normal_values(splits[13], (C2, 4 * C2), C2 ** -0.5, 0.375),
        "p_down": normal_values(splits[14], (4 * C2, C2), (4 * C2) ** -0.5, 0.1875),
        "p_gain": jnp.clip(1.0 + 0.18 * jax.random.normal(splits[15], (2, C2), jnp.float32), 0.1, 1.9),
        "unpool_w": normal_values(splits[16], (C2, C), C2 ** -0.5, 0.375),
    }


EPSILON = 1e-05
MASKED = -1e+30

def normed(values, weight_gain):
    average = lax.optimization_barrier(jnp.mean(values, axis=-1, keepdims=True))
    centred = values - average
    spread = lax.optimization_barrier(jnp.mean(centred * centred, axis=-1, keepdims=True))
    return (centred * lax.rsqrt(spread + EPSILON) * weight_gain).astype(jnp.bfloat16)

def attend_whole(packed, keep_mask):
    queries = packed[:, 0].astype(jnp.float32)
    keys_in = packed[:, 1].astype(jnp.float32)
    values_in = packed[:, 2].astype(jnp.float32)
    scores = jnp.einsum('qhd,khd->hqk', queries, keys_in) * (1.0 / math.sqrt(HEAD))
    scores = jnp.where(keep_mask[None, None, :], scores, MASKED)
    row_max = lax.optimization_barrier(jnp.max(scores, axis=-1, keepdims=True))
    exponent = jnp.exp(scores - row_max)
    weights = (exponent / lax.optimization_barrier(jnp.sum(exponent, axis=-1, keepdims=True))).astype(jnp.bfloat16)
    return jnp.einsum('hqk,khd->qhd', weights.astype(jnp.float32), values_in).astype(jnp.bfloat16)

def step_patch(inputs):
    return attend_whole(inputs[0], inputs[1])

def run_block(rows_in, keep_mask, gain_rows, w_qkv, w_proj, w_up, w_down):
    row_count, feature_width = rows_in.shape
    head_count = feature_width // HEAD
    rows_float = rows_in.astype(jnp.float32)
    normal_one = normed(rows_float, gain_rows[0])
    projected = jnp.dot(normal_one, w_qkv, preferred_element_type=jnp.float32).astype(jnp.bfloat16)
    projected = projected.reshape(row_count // PATCH, PATCH, 3, head_count, HEAD)
    keep_rows = keep_mask.reshape(row_count // PATCH, PATCH)
    attended = lax.map(step_patch, (projected, keep_rows)).reshape(row_count, feature_width)
    middle = rows_float + jnp.dot(attended, w_proj, preferred_element_type=jnp.float32)
    normal_two = normed(middle, gain_rows[1])
    hidden = jax.nn.gelu(jnp.dot(normal_two, w_up, preferred_element_type=jnp.float32), approximate=False).astype(jnp.bfloat16)
    return (middle + jnp.dot(hidden, w_down, preferred_element_type=jnp.float32)).astype(jnp.bfloat16)

def pick_rows(cell_rows, row_index):
    return cell_rows[row_index]

def reference(feats, z_count, hil_dest, pool_group, z_qkv, z_proj, z_up, z_down, z_gain, pool_w, bn_gain, p_qkv, p_proj, p_up, p_down, p_gain, unpool_w):
    cell_ids = jnp.arange(NCELLS).astype(jnp.int32)
    live_z = cell_ids % CELL_DEV < z_count[cell_ids // CELL_DEV]
    point_keep = jnp.repeat(live_z, CELL)
    z_out = run_block(feats.reshape(NCELLS * CELL, C), point_keep, z_gain, z_qkv, z_proj, z_up, z_down)
    z_out = z_out.reshape(NCELLS, CELL, C)
    h_cells = jnp.zeros_like(z_out).at[hil_dest].set(z_out)
    live_h = jnp.zeros((NCELLS,), dtype=bool).at[hil_dest].set(live_z)
    y_rows = jnp.dot(h_cells.reshape(NCELLS * CELL, C), pool_w, preferred_element_type=jnp.float32)
    group_ids = (cell_ids[:, None] * PGROUP + pool_group).reshape(-1)
    pooled_max = jax.ops.segment_max(y_rows, group_ids, num_segments=NCELLS * PGROUP)
    live_rows = jnp.repeat(live_h, PGROUP).astype(jnp.float32)[:, None]
    live_count = jnp.sum(live_rows)
    average = lax.optimization_barrier(jnp.sum(live_rows * pooled_max, axis=0)) / live_count
    variance = lax.optimization_barrier(jnp.sum(live_rows * (pooled_max - average) ** 2, axis=0)) / live_count
    pooled = jax.nn.gelu((pooled_max - average) * lax.rsqrt(variance + EPSILON) * bn_gain, approximate=False).astype(jnp.bfloat16)
    p_out = run_block(pooled, jnp.repeat(live_h, PGROUP), p_gain, p_qkv, p_proj, p_up, p_down)
    lifted = jnp.dot(p_out, unpool_w, preferred_element_type=jnp.float32).reshape(NCELLS, PGROUP, C)
    spread_back = jax.vmap(pick_rows)(lifted, pool_group)
    h_out = (h_cells.astype(jnp.float32) + spread_back).astype(jnp.bfloat16)
    return jnp.where(live_z[:, None, None], h_out[hil_dest], jnp.zeros((), jnp.bfloat16))
```

```python
import functools

import jax
import jax.numpy as jnp
from jax import lax
from jax.experimental import pallas as pl
from jax.experimental.pallas import tpu as pltpu
from jax.sharding import PartitionSpec as P

HEAD = 16
PGROUP = 32
PATCH = 1024
MOSTG = 8
LANES = 128
ROWS = 256
QROWS = 512
UNROLL = 2

EPSILON = 1e-05
MASKED = -1e30
BF = jnp.bfloat16
F32 = jnp.float32
VMEM = pl.BlockSpec(memory_space=pltpu.VMEM)
SMEM = pl.BlockSpec(memory_space=pltpu.SMEM)


def dot(a, b):
    return jnp.dot(a, b, preferred_element_type=F32)


def gelu(values):
    return 0.5 * values * (1.0 + lax.erf(values * (0.5**0.5)))


def normed(values, gain):
    average = jnp.mean(values, axis=-1, keepdims=True)
    centred = values - average
    spread = jnp.mean(centred * centred, axis=-1, keepdims=True)
    return (centred * lax.rsqrt(spread + EPSILON) * gain).astype(BF)


def lane_ids(rows):
    return lax.broadcasted_iota(jnp.int32, (rows, LANES), 1)


def attend(q_ref, k_ref, v_ref, att_ref):
    patch_rows = q_ref.shape[0]
    first_lane = (lane_ids(QROWS) == 0).astype(F32).astype(BF)
    blocks = patch_rows // QROWS

    def head_step(head, _):
        own = lane_ids(QROWS) // HEAD == head
        for block in range(blocks):
            rows = pl.ds(block * QROWS, QROWS)
            picked = jnp.where(own, q_ref[rows, :].astype(F32), 0.0).astype(BF)
            queries = jnp.concatenate([picked, first_lane], axis=1)
            scores = lax.dot_general(
                queries, k_ref[...], (((1,), (1,)), ((), ())), preferred_element_type=F32
            )
            top = jnp.max(scores, axis=-1, keepdims=True)
            weights = jnp.exp(scores - top).astype(BF)
            mixed = dot(weights, v_ref[...])
            att_ref[rows, :] = jnp.where(own, mixed[:, :LANES] / mixed[:, LANES:], att_ref[rows, :])
        return 0

    lax.fori_loop(0, LANES // HEAD, head_step, 0, unroll=UNROLL)


def block_body(
    load_rows, store_rows, bias_of, unit_rows, width, gain_ref, qkv_ref, proj_ref, up_ref, down_ref,
    q_scr, k_scr, v_scr, att_scr,
):
    slices = width // LANES
    chunks = PATCH // ROWS

    def project(chunk, _):
        rows = pl.ds(pl.multiple_of(chunk * ROWS, ROWS), ROWS)
        normal = normed(load_rows(chunk).astype(F32), gain_ref[0:1, :])
        packed = dot(normal, qkv_ref[...])
        for part in range(slices):
            start = part * LANES
            q_scr[part, rows, :] = (packed[:, start : start + LANES].astype(BF).astype(F32) * HEAD**-0.5).astype(BF)
            k_scr[part, rows, 0:LANES] = packed[:, width + start : width + start + LANES].astype(BF)
            v_scr[part, rows, 0:LANES] = packed[:, 2 * width + start : 2 * width + start + LANES].astype(BF)
            v_scr[part, rows, LANES:] = jnp.ones((ROWS, LANES), BF)
        return 0

    lax.fori_loop(0, chunks, project, 0)

    def mask_unit(unit, _):
        rows = pl.ds(pl.multiple_of(unit * unit_rows, unit_rows), unit_rows)
        bias = jnp.where(lane_ids(unit_rows) == 0, bias_of(unit), 0.0).astype(BF)
        for part in range(slices):
            k_scr[part, rows, LANES:] = bias
        return 0

    lax.fori_loop(0, PATCH // unit_rows, mask_unit, 0)

    for part in range(slices):
        attend(q_scr.at[part], k_scr.at[part], v_scr.at[part], att_scr.at[part])

    def finish(chunk, _):
        rows = pl.ds(pl.multiple_of(chunk * ROWS, ROWS), ROWS)
        attended = jnp.concatenate([att_scr[part, rows, :] for part in range(slices)], axis=1).astype(BF)
        middle = load_rows(chunk).astype(F32) + dot(attended, proj_ref[...])
        normal = normed(middle, gain_ref[1:2, :])
        hidden = gelu(dot(normal, up_ref[...])).astype(BF)
        store_rows(chunk, (middle + dot(hidden, down_ref[...])).astype(BF))
        return 0

    lax.fori_loop(0, chunks, finish, 0)


def block_scratch(width):
    slices = width // LANES
    return [
        pltpu.VMEM((slices, PATCH, LANES), BF),
        pltpu.VMEM((slices, PATCH, 2 * LANES), BF),
        pltpu.VMEM((slices, PATCH, 2 * LANES), BF),
        pltpu.VMEM((slices, PATCH, LANES), F32),
    ]


def params(**more):
    return pltpu.CompilerParams(vmem_limit_bytes=48 * 2**20, **more)


def block_cost(rows, width):
    flops = 2 * rows * (12 * width * width) + 4 * rows * PATCH * 256 * (width // HEAD)
    return pl.CostEstimate(
        flops=flops, bytes_accessed=4 * rows * width, transcendentals=rows * PATCH * (width // HEAD)
    )


def z_kernel(cell_points, count_ref, x_ref, gain, qkv, proj, up, down, out_ref, *scratch):
    first_cell = pl.program_id(0) * (PATCH // cell_points)

    def load_rows(chunk):
        return x_ref[pl.ds(pl.multiple_of(chunk * ROWS, ROWS), ROWS), :]

    def store_rows(chunk, rows):
        out_ref[pl.ds(pl.multiple_of(chunk * ROWS, ROWS), ROWS), :] = rows

    def bias_of(unit):
        return jnp.where(first_cell + unit < count_ref[0], 0.0, MASKED)

    block_body(load_rows, store_rows, bias_of, cell_points, x_ref.shape[1], gain, qkv, proj, up, down, *scratch)


def z_block(rows, z_count, cell_points, gain, qkv, proj, up, down):
    count, width = rows.shape
    return pl.pallas_call(
        functools.partial(z_kernel, cell_points),
        grid=(count // PATCH,),
        in_specs=[SMEM, pl.BlockSpec((PATCH, width), lambda i: (i, 0))] + [VMEM] * 5,
        out_specs=pl.BlockSpec((PATCH, width), lambda i: (i, 0)),
        out_shape=jax.ShapeDtypeStruct((count, width), BF),
        scratch_shapes=block_scratch(width),
        compiler_params=params(),
        cost_estimate=block_cost(count, width),
        name="z_block",
    )(z_count, rows, gain, qkv, proj, up, down)


def pool_kernel(count_ref, z_ref, group_ref, pool_ref, out_ref, stat_ref):
    cells, points, _ = z_ref.shape
    width = pool_ref.shape[1]
    groups = lax.broadcasted_iota(jnp.int32, (PGROUP, points), 0)
    lanes = lax.broadcasted_iota(jnp.int32, (PGROUP, points), 1)

    def one(cell, carry):
        total, square = carry
        own = jnp.broadcast_to(group_ref[pl.ds(cell, 1), :], (PGROUP, points))
        start = jnp.sum((own < groups).astype(F32), axis=1, keepdims=True).astype(jnp.int32)
        last = jnp.sum((own <= groups).astype(F32), axis=1, keepdims=True).astype(jnp.int32) - 1
        picks = jnp.concatenate(
            [(lanes == jnp.minimum(start + j, last)).astype(F32) for j in range(MOSTG)], axis=0
        ).astype(BF)
        chosen = dot(picks, z_ref[cell]).astype(BF)
        y = dot(chosen, pool_ref[...])
        top = y[0:PGROUP]
        for j in range(1, MOSTG):
            top = jnp.maximum(top, y[j * PGROUP : (j + 1) * PGROUP])
        out_ref[cell] = top
        kept = jnp.where(cell < count_ref[0], top, 0.0)
        return total + kept, square + kept * kept

    zero = jnp.zeros((PGROUP, width), F32)
    total, square = lax.fori_loop(0, cells, one, (zero, zero), unroll=2)
    stat_ref[0:1, :] = jnp.sum(total, axis=0, keepdims=True)
    stat_ref[1:2, :] = jnp.sum(square, axis=0, keepdims=True)


def pool(z_out, z_count, group_z, pool_w):
    cells = z_out.shape[0]
    width = pool_w.shape[1]
    return pl.pallas_call(
        pool_kernel,
        in_specs=[SMEM, VMEM, VMEM, VMEM],
        out_specs=[VMEM, VMEM],
        out_shape=[
            jax.ShapeDtypeStruct((cells, PGROUP, width), F32),
            jax.ShapeDtypeStruct((2, width), F32),
        ],
        compiler_params=params(),
        name="pool",
    )(z_count, z_out, group_z, pool_w)


def bn_kernel(position_ref, top_ref, scale_ref, out_ref):
    average = scale_ref[0:1, :]
    spread = scale_ref[1:2, :]
    gain = scale_ref[2:3, :]

    def one(cell, _):
        out_ref[position_ref[cell]] = gelu((top_ref[cell] - average) * spread * gain).astype(BF)
        return 0

    lax.fori_loop(0, top_ref.shape[0], one, 0, unroll=2)


def batch_norm(top, position, scales, slots):
    return pl.pallas_call(
        bn_kernel,
        in_specs=[SMEM, VMEM, VMEM],
        out_specs=VMEM,
        out_shape=jax.ShapeDtypeStruct((slots,) + top.shape[1:], BF),
        compiler_params=params(),
        name="batch_norm",
    )(position, top, scales)


def p_kernel(anchor_ref, live_ref, in_ref, gain, qkv, proj, up, down, unpool, out_ref, *scratch):
    per_chunk = ROWS // PGROUP
    first_cell = pl.program_id(0) * (PATCH // PGROUP)

    def load_rows(chunk):
        return jnp.concatenate(
            [in_ref[anchor_ref[first_cell + chunk * per_chunk + i]] for i in range(per_chunk)], axis=0
        )

    def store_rows(chunk, rows):
        lifted = dot(rows, unpool[...]).astype(BF)
        for i in range(per_chunk):
            out_ref[anchor_ref[first_cell + chunk * per_chunk + i]] = lifted[i * PGROUP : (i + 1) * PGROUP]

    def bias_of(unit):
        return jnp.where(live_ref[first_cell + unit] > 0, 0.0, MASKED)

    block_body(load_rows, store_rows, bias_of, PGROUP, in_ref.shape[2], gain, qkv, proj, up, down, *scratch)


def p_block(incoming, anchor, live, gain, qkv, proj, up, down, unpool):
    slots, _, width = incoming.shape
    rows = anchor.shape[0] * PGROUP
    return pl.pallas_call(
        p_kernel,
        grid=(rows // PATCH,),
        in_specs=[SMEM, SMEM] + [VMEM] * 7,
        out_specs=VMEM,
        out_shape=jax.ShapeDtypeStruct((slots, PGROUP, unpool.shape[1]), BF),
        scratch_shapes=block_scratch(width),
        compiler_params=params(),
        cost_estimate=block_cost(rows, width),
        name="p_block",
    )(anchor, live, incoming, gain, qkv, proj, up, down, unpool)


def final_kernel(position_ref, count_ref, z_ref, group_ref, back_ref, out_ref):
    cells, points, _ = z_ref.shape
    groups = lax.broadcasted_iota(jnp.int32, (PGROUP, points), 0)

    def one(cell, _):
        own = jnp.broadcast_to(group_ref[pl.ds(cell, 1), :], (PGROUP, points))
        pick = (own == groups).astype(F32).astype(BF)
        lifted = lax.dot_general(
            pick, back_ref[position_ref[cell]], (((0,), (0,)), ((), ())), preferred_element_type=F32
        )
        result = z_ref[cell].astype(F32) + lifted
        out_ref[cell] = jnp.where(cell < count_ref[0], result, 0.0).astype(BF)
        return 0

    lax.fori_loop(0, cells, one, 0, unroll=2)


def final(position, z_count, z_out, group_z, returned):
    return pl.pallas_call(
        final_kernel,
        in_specs=[SMEM, SMEM, VMEM, VMEM, VMEM],
        out_specs=VMEM,
        out_shape=jax.ShapeDtypeStruct(z_out.shape, BF),
        compiler_params=params(),
        name="final",
    )(position, z_count, z_out, group_z, returned)


def shards(
    feats, z_count, hil_dest, pool_group,
    z_qkv, z_proj, z_up, z_down, z_gain,
    pool_w, bn_gain,
    p_qkv, p_proj, p_up, p_down, p_gain,
    unpool_w,
):
    cells, points, width = feats.shape
    row_devices = lax.axis_size("gy")
    me = lax.axis_index("gy")
    capacity = 2 * cells // row_devices
    slots = row_devices * capacity
    cell_ids = jnp.arange(cells, dtype=jnp.int32)

    head = jnp.zeros((8, points), jnp.int32)
    head = head.at[0, :cells].set(hil_dest).at[1, 0].set(z_count[0])
    everyone = lax.all_gather(jnp.concatenate([head, pool_group], axis=0), "gy", axis=0, tiled=False)
    all_dest = everyone[:, 0, :cells]
    all_count = everyone[:, 1, 0]
    group_all = everyone[:, 8:, :].reshape(row_devices * cells, points)
    group_z = jnp.take(group_all, hil_dest % (row_devices * cells), axis=0)

    target = hil_dest // cells % row_devices
    earlier = cell_ids[None, :] < cell_ids[:, None]
    rank = jnp.sum(((target[:, None] == target[None, :]) & earlier).astype(jnp.int32), axis=1)
    position = target * capacity + rank

    mine = all_dest // cells % row_devices == me
    arrival = jnp.sum((mine[:, None, :] & earlier[None]).astype(jnp.int32), axis=2)
    arrival = arrival + jnp.arange(row_devices, dtype=jnp.int32)[:, None] * capacity
    alive = (cell_ids[None, :] < all_count[:, None]).astype(jnp.int32)
    match = mine[None] & (all_dest[None] % cells == cell_ids[:, None, None])
    anchor = jnp.sum(jnp.where(match, arrival[None], 0), axis=(1, 2))
    live_h = jnp.sum(jnp.where(match, alive[None], 0), axis=(1, 2))

    z_out = z_block(
        feats.reshape(cells * points, width), z_count, points, z_gain, z_qkv, z_proj, z_up, z_down
    ).reshape(cells, points, width)

    top, stats = pool(z_out, z_count, group_z, pool_w)
    live = jnp.full((1, stats.shape[1]), z_count[0] * PGROUP, F32)
    stats = lax.psum(jnp.concatenate([stats, live], axis=0), ("gx", "gy"))
    average = stats[0] / stats[2]
    variance = stats[1] / stats[2] - average * average
    scales = jnp.stack([average, lax.rsqrt(variance + EPSILON), bn_gain])
    outgoing = batch_norm(top, position, scales, slots)
    incoming = lax.all_to_all(outgoing, "gy", split_axis=0, concat_axis=0, tiled=True)
    lifted = p_block(incoming, anchor, live_h, p_gain, p_qkv, p_proj, p_up, p_down, unpool_w)
    returned = lax.all_to_all(lifted, "gy", split_axis=0, concat_axis=0, tiled=True)
    return final(position, z_count, z_out, group_z, returned)


def solution(mesh):
    shard = ("gx", "gy")
    in_specs = (P(shard, None, None), P(shard), P(shard), P(shard, None)) + (P(),) * 13
    return jax.shard_map(
        shards, mesh=mesh, in_specs=in_specs, out_specs=P(shard, None, None), check_vma=False
    )
```

```python
import functools

import jax
import jax.numpy as jnp
from jax import lax
from jax.experimental import pallas as pl
from jax.experimental.pallas import tpu as pltpu
from jax.sharding import PartitionSpec as P

HEAD = 16
PGROUP = 32
PATCH = 1024
MOSTG = 8
LANES = 128
ROWS = 256
QROWS = 512
UNROLL = 2

EPSILON = 1e-05
MASKED = -1e30
BF = jnp.bfloat16
F32 = jnp.float32
VMEM = pl.BlockSpec(memory_space=pltpu.VMEM)
SMEM = pl.BlockSpec(memory_space=pltpu.SMEM)


def dot(a, b):
    return jnp.dot(a, b, preferred_element_type=F32)


def gelu(values):
    return 0.5 * values * (1.0 + lax.erf(values * (0.5**0.5)))


def normed(values, gain):
    average = jnp.mean(values, axis=-1, keepdims=True)
    centred = values - average
    spread = jnp.mean(centred * centred, axis=-1, keepdims=True)
    return (centred * lax.rsqrt(spread + EPSILON) * gain).astype(BF)


def lane_ids(rows):
    return lax.broadcasted_iota(jnp.int32, (rows, LANES), 1)


def attend(q_ref, k_ref, v_ref, att_ref):
    patch_rows = q_ref.shape[0]
    first_lane = (lane_ids(QROWS) == 0).astype(F32).astype(BF)
    blocks = patch_rows // QROWS

    def head_step(head, _):
        own = lane_ids(QROWS) // HEAD == head
        for block in range(blocks):
            rows = pl.ds(block * QROWS, QROWS)
            picked = jnp.where(own, q_ref[rows, :].astype(F32), 0.0).astype(BF)
            queries = jnp.concatenate([picked, first_lane], axis=1)
            scores = lax.dot_general(
                queries, k_ref[...], (((1,), (1,)), ((), ())), preferred_element_type=F32
            )
            top = jnp.max(scores, axis=-1, keepdims=True)
            weights = jnp.exp(scores - top).astype(BF)
            mixed = dot(weights, v_ref[...])
            att_ref[rows, :] = jnp.where(own, mixed[:, :LANES] / mixed[:, LANES:], att_ref[rows, :])
        return 0

    lax.fori_loop(0, LANES // HEAD, head_step, 0, unroll=UNROLL)


def block_body(
    load_rows, store_rows, bias_of, unit_rows, width, gain_ref, qkv_ref, proj_ref, up_ref, down_ref,
    q_scr, k_scr, v_scr, att_scr,
):
    slices = width // LANES
    chunks = PATCH // ROWS

    def project(chunk, _):
        rows = pl.ds(pl.multiple_of(chunk * ROWS, ROWS), ROWS)
        normal = normed(load_rows(chunk).astype(F32), gain_ref[0:1, :])
        packed = dot(normal, qkv_ref[...])
        for part in range(slices):
            start = part * LANES
            q_scr[part, rows, :] = (packed[:, start : start + LANES].astype(BF).astype(F32) * HEAD**-0.5).astype(BF)
            k_scr[part, rows, 0:LANES] = packed[:, width + start : width + start + LANES].astype(BF)
            v_scr[part, rows, 0:LANES] = packed[:, 2 * width + start : 2 * width + start + LANES].astype(BF)
            v_scr[part, rows, LANES:] = jnp.ones((ROWS, LANES), BF)
        return 0

    lax.fori_loop(0, chunks, project, 0)

    def mask_unit(unit, _):
        rows = pl.ds(pl.multiple_of(unit * unit_rows, unit_rows), unit_rows)
        bias = jnp.where(lane_ids(unit_rows) == 0, bias_of(unit), 0.0).astype(BF)
        for part in range(slices):
            k_scr[part, rows, LANES:] = bias
        return 0

    lax.fori_loop(0, PATCH // unit_rows, mask_unit, 0)

    for part in range(slices):
        attend(q_scr.at[part], k_scr.at[part], v_scr.at[part], att_scr.at[part])

    def finish(chunk, _):
        rows = pl.ds(pl.multiple_of(chunk * ROWS, ROWS), ROWS)
        attended = jnp.concatenate([att_scr[part, rows, :] for part in range(slices)], axis=1).astype(BF)
        middle = load_rows(chunk).astype(F32) + dot(attended, proj_ref[...])
        normal = normed(middle, gain_ref[1:2, :])
        hidden = gelu(dot(normal, up_ref[...])).astype(BF)
        store_rows(chunk, (middle + dot(hidden, down_ref[...])).astype(BF))
        return 0

    lax.fori_loop(0, chunks, finish, 0)


def block_scratch(width):
    slices = width // LANES
    return [
        pltpu.VMEM((slices, PATCH, LANES), BF),
        pltpu.VMEM((slices, PATCH, 2 * LANES), BF),
        pltpu.VMEM((slices, PATCH, 2 * LANES), BF),
        pltpu.VMEM((slices, PATCH, LANES), F32),
    ]


def params(**more):
    return pltpu.CompilerParams(vmem_limit_bytes=48 * 2**20, **more)


def block_cost(rows, width):
    flops = 2 * rows * (12 * width * width) + 4 * rows * PATCH * 256 * (width // HEAD)
    return pl.CostEstimate(
        flops=flops, bytes_accessed=4 * rows * width, transcendentals=rows * PATCH * (width // HEAD)
    )


def z_kernel(cell_points, count_ref, x_ref, gain, qkv, proj, up, down, out_ref, *scratch):
    first_cell = pl.program_id(0) * (PATCH // cell_points)

    def load_rows(chunk):
        return x_ref[pl.ds(pl.multiple_of(chunk * ROWS, ROWS), ROWS), :]

    def store_rows(chunk, rows):
        out_ref[pl.ds(pl.multiple_of(chunk * ROWS, ROWS), ROWS), :] = rows

    def bias_of(unit):
        return jnp.where(first_cell + unit < count_ref[0], 0.0, MASKED)

    block_body(load_rows, store_rows, bias_of, cell_points, x_ref.shape[1], gain, qkv, proj, up, down, *scratch)


def z_block(rows, z_count, cell_points, gain, qkv, proj, up, down):
    count, width = rows.shape
    return pl.pallas_call(
        functools.partial(z_kernel, cell_points),
        grid=(count // PATCH,),
        in_specs=[SMEM, pl.BlockSpec((PATCH, width), lambda i: (i, 0))] + [VMEM] * 5,
        out_specs=pl.BlockSpec((PATCH, width), lambda i: (i, 0)),
        out_shape=jax.ShapeDtypeStruct((count, width), BF),
        scratch_shapes=block_scratch(width),
        compiler_params=params(),
        cost_estimate=block_cost(count, width),
        name="z_block",
    )(z_count, rows, gain, qkv, proj, up, down)


def pool_kernel(count_ref, z_ref, group_ref, pool_ref, out_ref, stat_ref):
    cells, points, _ = z_ref.shape
    width = pool_ref.shape[1]
    groups = lax.broadcasted_iota(jnp.int32, (PGROUP, points), 0)
    lanes = lax.broadcasted_iota(jnp.int32, (PGROUP, points), 1)

    def one(cell, carry):
        total, square = carry
        own = jnp.broadcast_to(group_ref[pl.ds(cell, 1), :], (PGROUP, points))
        start = jnp.sum((own < groups).astype(F32), axis=1, keepdims=True).astype(jnp.int32)
        last = jnp.sum((own <= groups).astype(F32), axis=1, keepdims=True).astype(jnp.int32) - 1
        picks = jnp.concatenate(
            [(lanes == jnp.minimum(start + j, last)).astype(F32) for j in range(MOSTG)], axis=0
        ).astype(BF)
        chosen = dot(picks, z_ref[cell]).astype(BF)
        y = dot(chosen, pool_ref[...])
        top = y[0:PGROUP]
        for j in range(1, MOSTG):
            top = jnp.maximum(top, y[j * PGROUP : (j + 1) * PGROUP])
        out_ref[cell] = top
        kept = jnp.where(cell < count_ref[0], top, 0.0)
        return total + kept, square + kept * kept

    zero = jnp.zeros((PGROUP, width), F32)
    total, square = lax.fori_loop(0, cells, one, (zero, zero), unroll=2)
    stat_ref[0:1, :] = jnp.sum(total, axis=0, keepdims=True)
    stat_ref[1:2, :] = jnp.sum(square, axis=0, keepdims=True)


def pool(z_out, z_count, group_z, pool_w):
    cells = z_out.shape[0]
    width = pool_w.shape[1]
    return pl.pallas_call(
        pool_kernel,
        in_specs=[SMEM, VMEM, VMEM, VMEM],
        out_specs=[VMEM, VMEM],
        out_shape=[
            jax.ShapeDtypeStruct((cells, PGROUP, width), F32),
            jax.ShapeDtypeStruct((2, width), F32),
        ],
        compiler_params=params(),
        name="pool",
    )(z_count, z_out, group_z, pool_w)


def bn_kernel(position_ref, top_ref, scale_ref, out_ref):
    average = scale_ref[0:1, :]
    spread = scale_ref[1:2, :]
    gain = scale_ref[2:3, :]

    def one(cell, _):
        out_ref[position_ref[cell]] = gelu((top_ref[cell] - average) * spread * gain).astype(BF)
        return 0

    lax.fori_loop(0, top_ref.shape[0], one, 0, unroll=2)


def batch_norm(top, position, scales, slots):
    return pl.pallas_call(
        bn_kernel,
        in_specs=[SMEM, VMEM, VMEM],
        out_specs=VMEM,
        out_shape=jax.ShapeDtypeStruct((slots,) + top.shape[1:], BF),
        compiler_params=params(),
        name="batch_norm",
    )(position, top, scales)


def p_kernel(anchor_ref, live_ref, in_ref, gain, qkv, proj, up, down, unpool, out_ref, *scratch):
    per_chunk = ROWS // PGROUP
    first_cell = pl.program_id(0) * (PATCH // PGROUP)

    def load_rows(chunk):
        return jnp.concatenate(
            [in_ref[anchor_ref[first_cell + chunk * per_chunk + i]] for i in range(per_chunk)], axis=0
        )

    def store_rows(chunk, rows):
        lifted = dot(rows, unpool[...]).astype(BF)
        for i in range(per_chunk):
            out_ref[anchor_ref[first_cell + chunk * per_chunk + i]] = lifted[i * PGROUP : (i + 1) * PGROUP]

    def bias_of(unit):
        return jnp.where(live_ref[first_cell + unit] > 0, 0.0, MASKED)

    block_body(load_rows, store_rows, bias_of, PGROUP, in_ref.shape[2], gain, qkv, proj, up, down, *scratch)


def p_block(incoming, anchor, live, gain, qkv, proj, up, down, unpool):
    slots, _, width = incoming.shape
    rows = anchor.shape[0] * PGROUP
    return pl.pallas_call(
        p_kernel,
        grid=(rows // PATCH,),
        in_specs=[SMEM, SMEM] + [VMEM] * 7,
        out_specs=VMEM,
        out_shape=jax.ShapeDtypeStruct((slots, PGROUP, unpool.shape[1]), BF),
        scratch_shapes=block_scratch(width),
        compiler_params=params(),
        cost_estimate=block_cost(rows, width),
        name="p_block",
    )(anchor, live, incoming, gain, qkv, proj, up, down, unpool)


def final_kernel(position_ref, count_ref, z_ref, group_ref, back_ref, out_ref):
    cells, points, _ = z_ref.shape
    groups = lax.broadcasted_iota(jnp.int32, (PGROUP, points), 0)

    def one(cell, _):
        own = jnp.broadcast_to(group_ref[pl.ds(cell, 1), :], (PGROUP, points))
        pick = (own == groups).astype(F32).astype(BF)
        lifted = lax.dot_general(
            pick, back_ref[position_ref[cell]], (((0,), (0,)), ((), ())), preferred_element_type=F32
        )
        result = z_ref[cell].astype(F32) + lifted
        out_ref[cell] = jnp.where(cell < count_ref[0], result, 0.0).astype(BF)
        return 0

    lax.fori_loop(0, cells, one, 0, unroll=2)


def final(position, z_count, z_out, group_z, returned):
    return pl.pallas_call(
        final_kernel,
        in_specs=[SMEM, SMEM, VMEM, VMEM, VMEM],
        out_specs=VMEM,
        out_shape=jax.ShapeDtypeStruct(z_out.shape, BF),
        compiler_params=params(),
        name="final",
    )(position, z_count, z_out, group_z, returned)


def coordinates(axes, sizes, index):
    ids = {}
    for axis, size in reversed(list(zip(axes, sizes))):
        ids[axis] = lax.rem(index, size)
        index = index // size
    return ids


def direct_kernel(axes, sizes, split, reduce, x_ref, out_ref, *scratch):
    *landing, send_sem, recv_sem = scratch
    slots = landing[0] if reduce else out_ref
    count = slots.shape[0]
    me = jnp.int32(0)
    for axis, size in zip(axes, sizes):
        me = me * size + lax.axis_index(axis)
    barrier = pltpu.get_barrier_semaphore()
    peers = [coordinates(axes, sizes, lax.rem(me + k, count)) for k in range(1, count)]
    for peer in peers:
        pl.semaphore_signal(barrier, inc=1, device_id=peer, device_id_type=pl.DeviceIdType.MESH)
    pl.semaphore_wait(barrier, count - 1)
    copies = []
    for k in range(1, count):
        copy = pltpu.make_async_remote_copy(
            src_ref=x_ref.at[lax.rem(me + k, count)] if split else x_ref,
            dst_ref=slots.at[me],
            send_sem=send_sem.at[k],
            recv_sem=recv_sem.at[k],
            device_id=peers[k - 1],
            device_id_type=pl.DeviceIdType.MESH,
        )
        copy.start()
        copies.append(copy)
    slots[me] = x_ref[me] if split else x_ref[...]
    for copy in copies:
        copy.wait()
    if reduce:
        out_ref[...] = jnp.sum(slots[...], axis=0)


def direct(x, axes, collective_id, split=False, reduce=False):
    sizes = [lax.axis_size(axis) for axis in axes]
    count = 1
    for size in sizes:
        count *= size
    shape = x.shape if split or reduce else (count,) + x.shape
    landing = [pltpu.VMEM((count,) + x.shape, x.dtype)] if reduce else []
    return pl.pallas_call(
        functools.partial(direct_kernel, axes, sizes, split, reduce),
        in_specs=[VMEM],
        out_specs=VMEM,
        out_shape=jax.ShapeDtypeStruct(shape, x.dtype),
        scratch_shapes=landing + [pltpu.SemaphoreType.DMA((count,)), pltpu.SemaphoreType.DMA((count,))],
        compiler_params=params(collective_id=collective_id, has_side_effects=True),
        name=f"direct_{collective_id}",
    )(x)


def shards(
    feats, z_count, hil_dest, pool_group,
    z_qkv, z_proj, z_up, z_down, z_gain,
    pool_w, bn_gain,
    p_qkv, p_proj, p_up, p_down, p_gain,
    unpool_w,
):
    cells, points, width = feats.shape
    row_devices = lax.axis_size("gy")
    me = lax.axis_index("gy")
    capacity = 2 * cells // row_devices
    slots = row_devices * capacity
    cell_ids = jnp.arange(cells, dtype=jnp.int32)

    head = jnp.zeros((8, points), jnp.int32)
    head = head.at[0, :cells].set(hil_dest).at[1, 0].set(z_count[0])
    everyone = direct(jnp.concatenate([head, pool_group], axis=0), ("gy",), 0)
    all_dest = everyone[:, 0, :cells]
    all_count = everyone[:, 1, 0]
    group_all = everyone[:, 8:, :].reshape(row_devices * cells, points)
    group_z = jnp.take(group_all, hil_dest % (row_devices * cells), axis=0)

    target = hil_dest // cells % row_devices
    earlier = cell_ids[None, :] < cell_ids[:, None]
    rank = jnp.sum(((target[:, None] == target[None, :]) & earlier).astype(jnp.int32), axis=1)
    position = target * capacity + rank

    mine = all_dest // cells % row_devices == me
    arrival = jnp.sum((mine[:, None, :] & earlier[None]).astype(jnp.int32), axis=2)
    arrival = arrival + jnp.arange(row_devices, dtype=jnp.int32)[:, None] * capacity
    alive = (cell_ids[None, :] < all_count[:, None]).astype(jnp.int32)
    match = mine[None] & (all_dest[None] % cells == cell_ids[:, None, None])
    anchor = jnp.sum(jnp.where(match, arrival[None], 0), axis=(1, 2))
    live_h = jnp.sum(jnp.where(match, alive[None], 0), axis=(1, 2))

    z_out = z_block(
        feats.reshape(cells * points, width), z_count, points, z_gain, z_qkv, z_proj, z_up, z_down
    ).reshape(cells, points, width)

    top, stats = pool(z_out, z_count, group_z, pool_w)
    live = jnp.full((6, stats.shape[1]), z_count[0] * PGROUP, F32)
    stats = direct(jnp.concatenate([stats, live], axis=0), ("gx", "gy"), 1, reduce=True)
    average = stats[0] / stats[2]
    variance = stats[1] / stats[2] - average * average
    scales = jnp.stack([average, lax.rsqrt(variance + EPSILON), bn_gain])
    outgoing = batch_norm(top, position, scales, slots)
    outgoing = outgoing.reshape((row_devices, capacity) + outgoing.shape[1:])
    incoming = direct(outgoing, ("gy",), 2, split=True).reshape((slots,) + outgoing.shape[2:])
    lifted = p_block(incoming, anchor, live_h, p_gain, p_qkv, p_proj, p_up, p_down, unpool_w)
    lifted = lifted.reshape((row_devices, capacity) + lifted.shape[1:])
    returned = direct(lifted, ("gy",), 3, split=True).reshape((slots,) + lifted.shape[2:])
    return final(position, z_count, z_out, group_z, returned)


def solution(mesh):
    shard = ("gx", "gy")
    in_specs = (P(shard, None, None), P(shard), P(shard), P(shard, None)) + (P(),) * 13
    return jax.shard_map(
        shards, mesh=mesh, in_specs=in_specs, out_specs=P(shard, None, None), check_vma=False
    )
```
